32 devices in a mesh: sp: 2 (over core), py: 4 (over z), pz: 4 (over y, x).
Axes of the slice: x: 2, y: 2, z: 4, core: 2. Of those that a mesh axis runs over, the one named last changes fastest.
Arguments:
- concentration: float32 [8, 128, 128, 128], P('sp', 'py', 'pz'), may hold values from -1 to 1.1
- mobility: float32 [8, 8], replicated, may hold values from 0.1 to 0.6
- kappa: float32 [8], replicated, may hold values from 0.5 to 2
- well_depth: float32 [8], P('sp'), may hold values from 0.5 to 2
Outputs:
- updated: float32 [8, 128, 128, 128], P('sp', 'py', 'pz')
The draws below stay inside these ranges and needn't reach their ends.
All inputs are finite; a program needn't handle non-finite values.
Results may differ from the reference program's by a relative error of at most 0.000084.
Values sent between devices are 32-bit elements; how exact they have to be, the bound alone decides.
A program may use at most 128 MiB of HBM per device.

```python
import math
import jax
import jax.numpy as jnp
from jax import lax

S = 8
NX = 128
NY = 128
NZ = 128


def draw_concentration(key, part):
    first = jax.random.fold_in(jax.random.fold_in(key, 11), 0)
    base = jax.random.uniform(first, (S, NX, NY, NZ), jnp.float32, -1.0, 1.0)
    return base


def level_of(own_key, extent, cuts, least, top_value):
    factor_of = 1.0
    for position, shards_of in cuts:
        draws = jax.random.uniform(jax.random.fold_in(jax.random.fold_in(own_key, 6), position), (shards_of,), jnp.float32, least / len(cuts), top_value / len(cuts))
        factor_of = factor_of * jnp.repeat(jnp.exp(draws), extent[position] // shards_of).reshape((-1,) + (1,) * (len(extent) - 1 - position))
    return factor_of


def setup_inputs(seed: int = 0) -> dict:
    seeds = jax.random.split(jax.random.key(seed), 5)
    return {
        "concentration": draw_concentration(jax.random.fold_in(seeds[4], 71), 0),
        "mobility": jnp.clip(jax.random.uniform(seeds[1], (S, S), jnp.float32, 0.1, 0.6), 0.1, 0.6),
        "kappa": jnp.clip(jnp.exp(jax.random.uniform(seeds[2], (S,), jnp.float32, math.log(0.5), math.log(2.0))), 0.5, 2.0),
        "well_depth": jnp.clip(jnp.exp(math.log(2.0) - 1.3862944 * jax.random.uniform(seeds[3], (S,), jnp.float32) ** level_of(seeds[3], (S,), ((0, 2),), -0.2, 0.2)), 0.5, 2.0),
    }


def wave_square(count):
    modes = jnp.arange(count, dtype=jnp.int32)
    freq = jnp.where(modes < count // 2, modes, modes - count).astype(jnp.float32)
    return (2.0 * math.pi * freq / count) ** 2


def reference(concentration, mobility, kappa, well_depth):
    conc = concentration
    bulk = well_depth[:, None, None, None] * (conc * conc * conc - conc)
    c_hat = jnp.fft.fftn(conc, axes=(1, 2, 3))
    bulk_hat = jnp.fft.fftn(bulk, axes=(1, 2, 3))
    ksq = wave_square(NX)[:, None, None] + wave_square(NY)[None, :, None] + wave_square(NZ)[None, None, :]
    drive = bulk_hat + kappa[:, None, None, None] * ksq[None] * c_hat
    mix_real = jnp.einsum("ij,jxyz->ixyz", mobility, jnp.real(drive), precision=lax.Precision.HIGHEST)
    mix_imag = jnp.einsum("ij,jxyz->ixyz", mobility, jnp.imag(drive), precision=lax.Precision.HIGHEST)
    mix = mix_real + 1j * mix_imag
    stiff = 0.5 * (jnp.diagonal(mobility) * kappa)[:, None, None, None] * (ksq * ksq)[None]
    new_hat = (c_hat * (1.0 + stiff) - 0.5 * ksq[None] * mix) / (1.0 + stiff)
    updated = jnp.real(jnp.fft.ifftn(new_hat, axes=(1, 2, 3)))
    return updated.astype(jnp.float32)
```

```python
import functools
import math

import jax
import jax.numpy as jnp
import numpy as np
from jax import lax
from jax.experimental import pallas as pl
from jax.experimental.pallas import tpu as pltpu
from jax.sharding import PartitionSpec as P


def tables(count):
    modes = jnp.arange(count, dtype=jnp.int32)
    product = modes[:, None] * modes[None, :] % count
    angle = 2.0 * math.pi * product.astype(jnp.float32) / count
    return (jnp.cos(angle), jnp.sin(angle))


def wave_square(index, count):
    freq = jnp.where(index < count // 2, index, index - count).astype(jnp.float32)
    return (2.0 * math.pi * freq / count) ** 2


def contract(form, values, table):
    return jnp.einsum(form, values, table, precision=lax.Precision.HIGHEST)


def rotate(spectrum, form, count, forward):
    cosine, sine = tables(count)
    real_part, imag_part = (spectrum[0], spectrum[1])
    real_cos = contract(form, real_part, cosine)
    real_sin = contract(form, real_part, sine)
    imag_cos = contract(form, imag_part, cosine)
    imag_sin = contract(form, imag_part, sine)
    if forward:
        return jnp.stack([real_cos + imag_sin, imag_cos - real_sin])
    return jnp.stack([real_cos - imag_sin, imag_cos + real_sin])


def per_device_general(concentration, mobility, kappa, well_depth):
    local_species, rows_x, rows_y, depth = concentration.shape
    count_sp = lax.axis_size("sp")
    count_py = lax.axis_size("py")
    count_pz = lax.axis_size("pz")
    full_x = rows_x * count_py
    full_y = rows_y * count_pz
    half_depth = depth // 2
    bulk = well_depth[:, None, None, None] * (
        concentration * concentration * concentration - concentration
    )
    fields = jnp.stack([concentration, bulk])
    cosine, sine = tables(depth)
    alternate = (1 - 2 * (jnp.arange(depth, dtype=jnp.int32) % 2)).astype(jnp.float32)
    spectrum = jnp.stack(
        [
            contract("fsxyz,zk->fsxyk", fields, cosine[:, :half_depth]),
            -contract("fsxyz,zk->fsxyk", fields, sine[:, :half_depth]),
        ]
    )
    spectrum = lax.all_to_all(spectrum, "pz", split_axis=5, concat_axis=4, tiled=True)
    own_lines = spectrum.shape[5]
    highest = contract("fsxyz,z->fsxy", fields, alternate)
    highest = lax.all_gather(highest, "pz", axis=3, tiled=True)
    highest = jnp.stack([highest, jnp.zeros_like(highest)])[..., None]
    spectrum = jnp.concatenate([spectrum, highest], axis=5)
    z_modes = jnp.concatenate(
        [
            lax.axis_index("pz") * own_lines + jnp.arange(own_lines, dtype=jnp.int32),
            jnp.full((1,), half_depth, jnp.int32),
        ]
    )
    spectrum = rotate(spectrum, "fsxyz,yk->fsxkz", full_y, True)
    spectrum = lax.all_to_all(
        lax.all_to_all(spectrum, "sp", split_axis=4, concat_axis=2, tiled=True),
        "py",
        split_axis=4,
        concat_axis=3,
        tiled=True,
    )
    spectrum = rotate(spectrum, "fsxyz,xk->fskyz", full_x, True)
    narrow = spectrum.shape[4]
    lines = spectrum.shape[5]
    y_start = (lax.axis_index("sp") * count_py + lax.axis_index("py")) * narrow
    ksq_x = wave_square(jnp.arange(full_x, dtype=jnp.int32), full_x)
    ksq_y = wave_square(y_start + jnp.arange(narrow, dtype=jnp.int32), full_y)
    ksq_z = wave_square(z_modes, depth)
    ksq = ksq_x[:, None, None] + ksq_y[None, :, None] + ksq_z[None, None, :]
    c_hat = spectrum[:, 0]
    drive = spectrum[:, 1] + kappa[None, :, None, None, None] * ksq[None, None] * c_hat
    mix = jnp.einsum("ij,rjxyz->rixyz", mobility, drive, precision=lax.Precision.HIGHEST)
    stiff = 0.5 * (jnp.diagonal(mobility) * kappa)[:, None, None, None] * (ksq * ksq)[None]
    new_hat = (c_hat * (1.0 + stiff)[None] - 0.5 * ksq[None, None] * mix) / (1.0 + stiff)[None]
    new_hat = rotate(new_hat, "sxyz,xk->skyz", full_x, False)
    moved = lax.all_to_all(
        lax.all_to_all(new_hat, "sp", split_axis=1, concat_axis=3, tiled=True),
        "py",
        split_axis=2,
        concat_axis=3,
        tiled=True,
    )
    moved = moved.reshape(2, local_species, rows_x, count_py, count_sp, narrow, lines)
    moved = moved.transpose(0, 1, 2, 4, 3, 5, 6).reshape(2, local_species, rows_x, full_y, lines)
    moved = rotate(moved, "sxyz,yk->sxkz", full_y, False)
    main = moved[..., : lines - 1]
    highest = moved[0, :, :, :, lines - 1]
    main = lax.all_to_all(main, "pz", split_axis=3, concat_axis=4, tiled=True)
    highest = lax.dynamic_slice_in_dim(highest, lax.axis_index("pz") * rows_y, rows_y, 2)
    weight = jnp.where(jnp.arange(half_depth, dtype=jnp.int32) == 0, 1.0, 2.0).astype(jnp.float32)
    result = contract("sxyk,kz->sxyz", main[0] * weight, cosine[:half_depth]) - contract(
        "sxyk,kz->sxyz", main[1] * weight, sine[:half_depth]
    )
    result = result + highest[..., None] * alternate[None, None, None, :]
    return result * (1.0 / (full_x * full_y * depth))


def basis(count):
    grid = np.arange(count)
    mode = np.arange(count)
    freq = np.minimum(mode, count - mode)
    angle = 2.0 * np.pi * (grid[:, None] * freq[None, :] % count) / count
    table = np.where(mode[None, :] <= count // 2, np.cos(angle), np.sin(angle))
    single = (mode == 0) | (2 * mode == count)
    return table * np.sqrt(np.where(single, 1.0, 2.0) / count)[None, :]


def split_table(table):
    table = table.astype(np.float32)
    high = table.astype(jnp.bfloat16)
    low = (table - high.astype(np.float32)).astype(jnp.bfloat16)
    row = np.concatenate([high, low], axis=1)
    return np.concatenate([row, row], axis=0)


def split(values, axis):
    high = values.astype(jnp.bfloat16)
    low = (values - high.astype(jnp.float32)).astype(jnp.bfloat16)
    return jnp.concatenate([high, low], axis=axis)


def from_right(values, table):
    count = values.shape[1]
    out = jnp.dot(split(values, 1), table, preferred_element_type=jnp.float32)
    return out[:, :count] + out[:, count:]


def from_left(table, values):
    count = values.shape[0]
    out = jnp.dot(table, split(values, 0), preferred_element_type=jnp.float32)
    return out[:count] + out[count:]


def swap_blocks(parts, width):
    parts = list(parts)
    axis = parts[0].ndim - 1
    lanes = parts[0].shape[axis]
    block = lax.broadcasted_iota(jnp.int32, parts[0].shape, axis) // width
    half = len(parts) // 2
    while half:
        low_side = (block // half) % 2 == 0
        for first in range(len(parts)):
            if (first // half) % 2 == 0:
                one, two = parts[first], parts[first + half]
                parts[first] = jnp.where(low_side, one, pltpu.roll(two, half * width, axis))
                parts[first + half] = jnp.where(
                    low_side, pltpu.roll(one, lanes - half * width, axis), two
                )
        half //= 2
    return parts


def kernel(
    sizes, conc, mobility, kappa, depths, right_f, right_i, left_f, left_i, out,
    other, other_depths, z_out, z_in, y_out, y_in, x_out, x_in, w_out, w_in,
    pair_send, pair_recv, zs, zr, ys, yr, xs, xr, ws, wr,
):
    count_py, count_pz = sizes
    species, rows_x, rows_y, n = conc.shape
    me_sp, me_py, me_pz = lax.axis_index("sp"), lax.axis_index("py"), lax.axis_index("pz")
    width = n // count_pz
    groups = rows_x // count_pz
    own_ky = n // count_py
    sub = own_ky // count_pz
    strip = rows_x * sub
    mesh_id = pl.DeviceIdType.MESH

    def along_py(step):
        return {"sp": me_sp, "py": lax.rem(me_py + step, count_py), "pz": me_pz}

    def along_pz(step):
        return {"sp": me_sp, "py": me_py, "pz": lax.rem(me_pz + step, count_pz)}

    partner = {"sp": 1 - me_sp, "py": me_py, "pz": me_pz}
    barrier = pltpu.get_barrier_semaphore()
    peers = [partner]
    peers += [along_pz(step) for step in range(1, count_pz)]
    peers += [along_py(step) for step in range(1, count_py)]
    for peer in peers:
        pl.semaphore_signal(barrier, inc=1, device_id=peer, device_id_type=mesh_id)
    pl.semaphore_wait(barrier, len(peers))

    def remote(source, target, send, recv, peer):
        return pltpu.make_async_remote_copy(
            src_ref=source, dst_ref=target, send_sem=send, recv_sem=recv,
            device_id=peer, device_id_type=mesh_id,
        )

    pair = [
        remote(depths, other_depths, pair_send.at[0], pair_recv.at[0], partner),
        remote(conc, other, pair_send.at[1], pair_recv.at[1], partner),
    ]
    for copy in pair:
        copy.start()

    y_rows = pl.ds(pl.multiple_of(me_pz * rows_y, rows_y), rows_y)
    x_rows = pl.ds(pl.multiple_of(me_py * strip, strip), strip)

    def z_copy(chunk, step):
        peer = lax.rem(me_pz + step, count_pz)
        return remote(
            z_out.at[chunk, peer], z_in.at[chunk, :, y_rows], zs.at[chunk, step],
            zr.at[chunk, step], along_pz(step),
        )

    def y_copy(chunk, step):
        peer = lax.rem(me_py + step, count_py)
        return remote(
            y_out.at[chunk, peer], y_in.at[chunk, x_rows], ys.at[chunk, step],
            yr.at[chunk, step], along_py(step),
        )

    def x_copy(one, step):
        peer = lax.rem(me_py + step, count_py)
        rows = pl.ds(pl.multiple_of(peer * strip, strip), strip)
        return remote(
            x_out.at[one, rows], x_in.at[one, me_py], xs.at[one, step],
            xr.at[one, step], along_py(step),
        )

    def w_copy(one, step):
        peer = lax.rem(me_pz + step, count_pz)
        return remote(
            w_out.at[one, peer], w_in.at[one, me_pz], ws.at[one, step],
            wr.at[one, step], along_pz(step),
        )

    for copy in pair:
        copy.wait_recv()

    def z_forward(one, _):
        own_i = me_sp * species + one
        terms = []
        for side, field, depth in ((me_sp, conc, depths), (1 - me_sp, other, other_depths)):
            for t in range(species):
                j = side * species + t
                weight = mobility[own_i, j]
                terms.append((field, t, weight * depth[t : t + 1, :], weight * kappa[j]))
        for g in range(groups):
            bulk_mix, conc_mix = [], []
            for block in range(count_pz):
                first = second = None
                for field, t, bulk_weight, conc_weight in terms:
                    c = field[t, block * groups + g]
                    a = bulk_weight * (c * c * c - c)
                    b = conc_weight * c
                    first = a if first is None else first + a
                    second = b if second is None else second + b
                bulk_mix.append(first)
                conc_mix.append(second)
            modes = from_right(jnp.concatenate(bulk_mix + conc_mix, axis=0), right_f[...])
            modes = modes.reshape(2, count_pz, rows_y, n)
            for f in range(2):
                swapped = swap_blocks([modes[f, block] for block in range(count_pz)], width)
                for q in range(count_pz):
                    z_out[2 * one + f, q, g] = swapped[q]
        for f in range(2):
            for step in range(1, count_pz):
                z_copy(2 * one + f, step).start()
        for f in range(2):
            z_in[2 * one + f, :, y_rows] = z_out[2 * one + f, me_pz]
        return 0

    lax.fori_loop(0, species, z_forward, 0)

    def y_forward(chunk, _):
        for step in range(1, count_pz):
            z_copy(chunk, step).wait_recv()
        for g in range(0, groups, 2):
            lines = jnp.concatenate([z_in[chunk, g], z_in[chunk, g + 1]], axis=1)
            modes = from_left(left_f[...], lines)
            for h in range(2):
                part = modes[:, h * n : (h + 1) * n].reshape(count_py, count_pz, sub, n)
                swapped = swap_blocks([part[:, b] for b in range(count_pz)], width)
                for block in range(count_pz):
                    start = (block * groups + g + h) * sub
                    y_out[chunk, :, start : start + sub, :] = swapped[block]
        for step in range(1, count_py):
            y_copy(chunk, step).start()
        y_in[chunk, x_rows] = y_out[chunk, me_py]
        return 0

    lax.fori_loop(0, 2 * species, y_forward, 0)

    def square(index):
        freq = jnp.minimum(index, n - index).astype(jnp.float32)
        root = freq * (2.0 * math.pi / n)
        return root * root

    lane = lax.broadcasted_iota(jnp.int32, (1, n), 1)
    ksq_x = square(lax.broadcasted_iota(jnp.int32, (n, 1), 0))
    ksq_z = square(me_pz * width + lane % width)

    def x_both(one, _):
        for f in range(2):
            for step in range(1, count_py):
                y_copy(2 * one + f, step).wait_recv()
        own_i = me_sp * species + one
        half_stiff = 0.5 * (mobility[own_i, own_i] * kappa[own_i])
        for r in range(0, sub, 2):
            both, ksq = [], []
            for f in range(2):
                both.append(from_left(left_f[...], jnp.concatenate(
                    [y_in[2 * one + f, pl.ds(r + h, n, stride=sub), :] for h in range(2)], axis=1
                )))
            for h in range(2):
                ksq_y = square(me_py * own_ky + (lane // width) * sub + (r + h))
                ksq.append(ksq_x + (ksq_y + ksq_z))
            ksq = jnp.concatenate(ksq, axis=1)
            drop = 0.5 * ksq * (both[0] + ksq * both[1]) / (1.0 + half_stiff * (ksq * ksq))
            lines = from_left(left_i[...], drop)
            for h in range(2):
                x_out[one, pl.ds(r + h, n, stride=sub), :] = lines[:, h * n : (h + 1) * n]
        for step in range(1, count_py):
            x_copy(one, step).start()
        x_in[one, me_py] = x_out[one, x_rows]
        return 0

    lax.fori_loop(0, species, x_both, 0)

    def y_back(one, _):
        for step in range(1, count_py):
            x_copy(one, step).wait_recv()
        for g in range(0, groups, 2):
            pairs = []
            for h in range(2):
                parts = []
                for block in range(count_pz):
                    start = (block * groups + g + h) * sub
                    parts.append(x_in[one, :, start : start + sub, :])
                swapped = swap_blocks(parts, width)
                pairs.append(jnp.stack(swapped, axis=1).reshape(n, n))
            lines = from_left(left_i[...], jnp.concatenate(pairs, axis=1))
            for h in range(2):
                part = lines[:, h * n : (h + 1) * n].reshape(count_pz, rows_y, n)
                w_out[one, :, g + h] = part
        for step in range(1, count_pz):
            w_copy(one, step).start()
        w_in[one, me_pz] = w_out[one, me_pz]
        return 0

    lax.fori_loop(0, species, y_back, 0)

    def z_back(one, _):
        for step in range(1, count_pz):
            w_copy(one, step).wait_recv()
        for g in range(0, groups, 2):
            rows = []
            for h in range(2):
                rows += swap_blocks([w_in[one, q, g + h] for q in range(count_pz)], width)
            lines = from_right(jnp.concatenate(rows, axis=0), right_i[...])
            lines = lines.reshape(2, count_pz, rows_y, n)
            for h in range(2):
                for block in range(count_pz):
                    x = block * groups + g + h
                    out[one, x] = conc[one, x] - lines[h, block]
        return 0

    lax.fori_loop(0, species, z_back, 0)

    for copy in pair:
        copy.wait_send()

    def drain(one, _):
        for step in range(1, count_pz):
            z_copy(2 * one, step).wait_send()
            z_copy(2 * one + 1, step).wait_send()
            w_copy(one, step).wait_send()
        for step in range(1, count_py):
            y_copy(2 * one, step).wait_send()
            y_copy(2 * one + 1, step).wait_send()
            x_copy(one, step).wait_send()
        return 0

    lax.fori_loop(0, species, drain, 0)


def per_device_kernel(concentration, mobility, kappa, well_depth):
    species, rows_x, rows_y, n = concentration.shape
    count_py, count_pz = lax.axis_size("py"), lax.axis_size("pz")
    forward = split_table(basis(n))
    inverse = split_table(basis(n).T)
    depths = jnp.broadcast_to(well_depth[:, None], (species, n))
    groups = rows_x // count_pz
    sub = n // count_py // count_pz
    strip = rows_x * sub
    f32 = jnp.float32
    vmem = pl.BlockSpec(memory_space=pltpu.VMEM)
    smem = pl.BlockSpec(memory_space=pltpu.SMEM)
    dma = pltpu.SemaphoreType.DMA
    return pl.pallas_call(
        functools.partial(kernel, (count_py, count_pz)),
        out_shape=jax.ShapeDtypeStruct(concentration.shape, f32),
        in_specs=[vmem, smem, smem, vmem, vmem, vmem, vmem, vmem],
        out_specs=vmem,
        scratch_shapes=[
            pltpu.VMEM((species, rows_x, rows_y, n), f32),
            pltpu.VMEM((species, n), f32),
            pltpu.VMEM((2 * species, count_pz, groups, rows_y, n), f32),
            pltpu.VMEM((2 * species, groups, n, n), f32),
            pltpu.VMEM((2 * species, count_py, strip, n), f32),
            pltpu.VMEM((2 * species, n * sub, n), f32),
            pltpu.VMEM((species, n * sub, n), f32),
            pltpu.VMEM((species, count_py, strip, n), f32),
            pltpu.VMEM((species, count_pz, groups, rows_y, n), f32),
            pltpu.VMEM((species, count_pz, groups, rows_y, n), f32),
            dma((2,)), dma((2,)),
            dma((2 * species, count_pz)), dma((2 * species, count_pz)),
            dma((2 * species, count_py)), dma((2 * species, count_py)),
            dma((species, count_py)), dma((species, count_py)),
            dma((species, count_pz)), dma((species, count_pz)),
        ],
        compiler_params=pltpu.CompilerParams(
            collective_id=0, has_side_effects=True, vmem_limit_bytes=60 * 1024 * 1024
        ),
        name="step",
    )(
        concentration, mobility, kappa, depths,
        jnp.asarray(forward), jnp.asarray(inverse),
        jnp.asarray(forward.T), jnp.asarray(inverse.T),
    )


def per_device(concentration, mobility, kappa, well_depth):
    rows_x, rows_y, n = concentration.shape[1:]
    count_sp, count_py, count_pz = (lax.axis_size(name) for name in ("sp", "py", "pz"))
    cube = rows_x * count_py == n and rows_y * count_pz == n and n == 128
    power = count_pz > 1 and count_pz & (count_pz - 1) == 0
    whole = n % (8 * count_py * count_pz) == 0 and rows_x % (2 * count_pz) == 0 and rows_y % 8 == 0
    if cube and power and whole and count_sp == 2:
        return per_device_kernel(concentration, mobility, kappa, well_depth)
    return per_device_general(concentration, mobility, kappa, well_depth)


def solution(mesh):
    in_specs = (P("sp", "py", "pz", None), P(), P(), P("sp"))
    out_specs = P("sp", "py", "pz", None)
    return jax.shard_map(
        per_device, mesh=mesh, in_specs=in_specs, out_specs=out_specs, check_vma=False
    )
```

```python
import functools
import math

import jax
import jax.numpy as jnp
import numpy as np
from jax import lax
from jax.experimental import pallas as pl
from jax.experimental.pallas import tpu as pltpu
from jax.sharding import PartitionSpec as P


def tables(count):
    modes = jnp.arange(count, dtype=jnp.int32)
    product = modes[:, None] * modes[None, :] % count
    angle = 2.0 * math.pi * product.astype(jnp.float32) / count
    return (jnp.cos(angle), jnp.sin(angle))


def wave_square(index, count):
    freq = jnp.where(index < count // 2, index, index - count).astype(jnp.float32)
    return (2.0 * math.pi * freq / count) ** 2


def contract(form, values, table):
    return jnp.einsum(form, values, table, precision=lax.Precision.HIGHEST)


def rotate(spectrum, form, count, forward):
    cosine, sine = tables(count)
    real_part, imag_part = (spectrum[0], spectrum[1])
    real_cos = contract(form, real_part, cosine)
    real_sin = contract(form, real_part, sine)
    imag_cos = contract(form, imag_part, cosine)
    imag_sin = contract(form, imag_part, sine)
    if forward:
        return jnp.stack([real_cos + imag_sin, imag_cos - real_sin])
    return jnp.stack([real_cos - imag_sin, imag_cos + real_sin])


def per_device_general(concentration, mobility, kappa, well_depth):
    local_species, rows_x, rows_y, depth = concentration.shape
    count_sp = lax.axis_size("sp")
    count_py = lax.axis_size("py")
    count_pz = lax.axis_size("pz")
    full_x = rows_x * count_py
    full_y = rows_y * count_pz
    half_depth = depth // 2
    bulk = well_depth[:, None, None, None] * (
        concentration * concentration * concentration - concentration
    )
    fields = jnp.stack([concentration, bulk])
    cosine, sine = tables(depth)
    alternate = (1 - 2 * (jnp.arange(depth, dtype=jnp.int32) % 2)).astype(jnp.float32)
    spectrum = jnp.stack(
        [
            contract("fsxyz,zk->fsxyk", fields, cosine[:, :half_depth]),
            -contract("fsxyz,zk->fsxyk", fields, sine[:, :half_depth]),
        ]
    )
    spectrum = lax.all_to_all(spectrum, "pz", split_axis=5, concat_axis=4, tiled=True)
    own_lines = spectrum.shape[5]
    highest = contract("fsxyz,z->fsxy", fields, alternate)
    highest = lax.all_gather(highest, "pz", axis=3, tiled=True)
    highest = jnp.stack([highest, jnp.zeros_like(highest)])[..., None]
    spectrum = jnp.concatenate([spectrum, highest], axis=5)
    z_modes = jnp.concatenate(
        [
            lax.axis_index("pz") * own_lines + jnp.arange(own_lines, dtype=jnp.int32),
            jnp.full((1,), half_depth, jnp.int32),
        ]
    )
    spectrum = rotate(spectrum, "fsxyz,yk->fsxkz", full_y, True)
    spectrum = lax.all_to_all(
        lax.all_to_all(spectrum, "sp", split_axis=4, concat_axis=2, tiled=True),
        "py",
        split_axis=4,
        concat_axis=3,
        tiled=True,
    )
    spectrum = rotate(spectrum, "fsxyz,xk->fskyz", full_x, True)
    narrow = spectrum.shape[4]
    lines = spectrum.shape[5]
    y_start = (lax.axis_index("sp") * count_py + lax.axis_index("py")) * narrow
    ksq_x = wave_square(jnp.arange(full_x, dtype=jnp.int32), full_x)
    ksq_y = wave_square(y_start + jnp.arange(narrow, dtype=jnp.int32), full_y)
    ksq_z = wave_square(z_modes, depth)
    ksq = ksq_x[:, None, None] + ksq_y[None, :, None] + ksq_z[None, None, :]
    c_hat = spectrum[:, 0]
    drive = spectrum[:, 1] + kappa[None, :, None, None, None] * ksq[None, None] * c_hat
    mix = jnp.einsum("ij,rjxyz->rixyz", mobility, drive, precision=lax.Precision.HIGHEST)
    stiff = 0.5 * (jnp.diagonal(mobility) * kappa)[:, None, None, None] * (ksq * ksq)[None]
    new_hat = (c_hat * (1.0 + stiff)[None] - 0.5 * ksq[None, None] * mix) / (1.0 + stiff)[None]
    new_hat = rotate(new_hat, "sxyz,xk->skyz", full_x, False)
    moved = lax.all_to_all(
        lax.all_to_all(new_hat, "sp", split_axis=1, concat_axis=3, tiled=True),
        "py",
        split_axis=2,
        concat_axis=3,
        tiled=True,
    )
    moved = moved.reshape(2, local_species, rows_x, count_py, count_sp, narrow, lines)
    moved = moved.transpose(0, 1, 2, 4, 3, 5, 6).reshape(2, local_species, rows_x, full_y, lines)
    moved = rotate(moved, "sxyz,yk->sxkz", full_y, False)
    main = moved[..., : lines - 1]
    highest = moved[0, :, :, :, lines - 1]
    main = lax.all_to_all(main, "pz", split_axis=3, concat_axis=4, tiled=True)
    highest = lax.dynamic_slice_in_dim(highest, lax.axis_index("pz") * rows_y, rows_y, 2)
    weight = jnp.where(jnp.arange(half_depth, dtype=jnp.int32) == 0, 1.0, 2.0).astype(jnp.float32)
    result = contract("sxyk,kz->sxyz", main[0] * weight, cosine[:half_depth]) - contract(
        "sxyk,kz->sxyz", main[1] * weight, sine[:half_depth]
    )
    result = result + highest[..., None] * alternate[None, None, None, :]
    return result * (1.0 / (full_x * full_y * depth))


def basis(count):
    grid = np.arange(count)
    mode = np.arange(count)
    freq = np.minimum(mode, count - mode)
    angle = 2.0 * np.pi * (grid[:, None] * freq[None, :] % count) / count
    table = np.where(mode[None, :] <= count // 2, np.cos(angle), np.sin(angle))
    single = (mode == 0) | (2 * mode == count)
    return table * np.sqrt(np.where(single, 1.0, 2.0) / count)[None, :]


def split_table(table):
    table = table.astype(np.float32)
    high = table.astype(jnp.bfloat16)
    low = (table - high.astype(np.float32)).astype(jnp.bfloat16)
    row = np.concatenate([high, low], axis=1)
    return np.concatenate([row, row], axis=0)


def split(values, axis):
    high = values.astype(jnp.bfloat16)
    low = (values - high.astype(jnp.float32)).astype(jnp.bfloat16)
    return jnp.concatenate([high, low], axis=axis)


def from_right(values, table):
    count = values.shape[1]
    out = jnp.dot(split(values, 1), table, preferred_element_type=jnp.float32)
    return out[:, :count] + out[:, count:]


def from_left(table, values):
    count = table.shape[0] // 2
    out = jnp.dot(table, split(values, 0), preferred_element_type=jnp.float32)
    return out[:count] + out[count:]


def swap_blocks(parts, width):
    parts = list(parts)
    axis = parts[0].ndim - 1
    lanes = parts[0].shape[axis]
    block = lax.broadcasted_iota(jnp.int32, parts[0].shape, axis) // width
    half = len(parts) // 2
    while half:
        low_side = (block // half) % 2 == 0
        for first in range(len(parts)):
            if (first // half) % 2 == 0:
                one, two = parts[first], parts[first + half]
                parts[first] = jnp.where(low_side, one, pltpu.roll(two, half * width, axis))
                parts[first + half] = jnp.where(
                    low_side, pltpu.roll(one, lanes - half * width, axis), two
                )
        half //= 2
    return parts


def kernel(
    sizes, conc, mobility, kappa, depths, right_f, right_i, left_f, left_i, half_f, half_i, out,
    other, other_depths, z_out, z_in, y_out, y_in, near, x_out, x_in, b_out, b_in, w_out, w_in,
    pair_send, pair_recv, zs, zr, ys, yr, xs, xr, bs, br, ws, wr,
):
    count_py, count_pz = sizes
    species, rows_x, rows_y, n = conc.shape
    me_sp, me_py, me_pz = lax.axis_index("sp"), lax.axis_index("py"), lax.axis_index("pz")
    width = n // count_pz
    groups = rows_x // count_pz
    slabs = count_py
    slab_ky = n // slabs
    sub = slab_ky // count_pz
    strip = rows_x * sub
    mesh_id = pl.DeviceIdType.MESH

    half = me_py // 2
    inner = lax.rem(me_py + half, 2) == 1
    outer = jnp.logical_not(inner)
    buddy = {"sp": me_sp, "py": me_py + 1 - 2 * lax.rem(me_py, 2), "pz": me_pz}
    across = {"sp": me_sp, "py": count_py - 1 - me_py, "pz": me_pz}

    def along_pz(step):
        return {"sp": me_sp, "py": me_py, "pz": lax.rem(me_pz + step, count_pz)}

    partner = {"sp": 1 - me_sp, "py": me_py, "pz": me_pz}
    barrier = pltpu.get_barrier_semaphore()
    peers = [partner, buddy, across]
    peers += [along_pz(step) for step in range(1, count_pz)]
    for peer in peers:
        pl.semaphore_signal(barrier, inc=1, device_id=peer, device_id_type=mesh_id)
    pl.semaphore_wait(barrier, len(peers))

    def remote(source, target, send, recv, peer):
        return pltpu.make_async_remote_copy(
            src_ref=source, dst_ref=target, send_sem=send, recv_sem=recv,
            device_id=peer, device_id_type=mesh_id,
        )

    pair = [
        remote(depths, other_depths, pair_send.at[0], pair_recv.at[0], partner),
        remote(conc, other, pair_send.at[1], pair_recv.at[1], partner),
    ]
    for copy in pair:
        copy.start()

    y_rows = pl.ds(pl.multiple_of(me_pz * rows_y, rows_y), rows_y)

    def z_copy(chunk, step):
        peer = lax.rem(me_pz + step, count_pz)
        return remote(
            z_out.at[chunk, peer], z_in.at[chunk, :, y_rows], zs.at[chunk, step],
            zr.at[chunk, step], along_pz(step),
        )

    def y_copy(chunk, slab):
        return remote(
            y_out.at[chunk, slab], y_in.at[chunk, slab], ys.at[chunk, slab],
            yr.at[chunk, slab], buddy,
        )

    def x_copy(one, slab):
        return remote(
            x_out.at[one, slab], x_in.at[one, slab], xs.at[one, slab], xr.at[one, slab], across
        )

    def b_copy(one, slab):
        return remote(
            b_out.at[one, slab], b_in.at[one, slab], bs.at[one, slab], br.at[one, slab], buddy
        )

    def w_copy(one, step):
        peer = lax.rem(me_pz + step, count_pz)
        return remote(
            w_out.at[one, peer], w_in.at[one, me_pz], ws.at[one, step],
            wr.at[one, step], along_pz(step),
        )

    for copy in pair:
        copy.wait_recv()

    def z_forward(one):
        own_i = me_sp * species + one
        terms = []
        for side, field, depth in ((me_sp, conc, depths), (1 - me_sp, other, other_depths)):
            for t in range(species):
                j = side * species + t
                weight = mobility[own_i, j]
                terms.append((field, t, weight * depth[t : t + 1, :], weight * kappa[j]))
        for g in range(groups):
            bulk_mix, conc_mix = [], []
            for block in range(count_pz):
                first = second = None
                for field, t, bulk_weight, conc_weight in terms:
                    c = field[t, block * groups + g]
                    a = bulk_weight * (c * c * c - c)
                    b = conc_weight * c
                    first = a if first is None else first + a
                    second = b if second is None else second + b
                bulk_mix.append(first)
                conc_mix.append(second)
            modes = from_right(jnp.concatenate(bulk_mix + conc_mix, axis=0), right_f[...])
            modes = modes.reshape(2, count_pz, rows_y, n)
            for f in range(2):
                swapped = swap_blocks([modes[f, block] for block in range(count_pz)], width)
                for q in range(count_pz):
                    z_out[2 * one + f, q, g] = swapped[q]
        for f in range(2):
            for step in range(1, count_pz):
                z_copy(2 * one + f, step).start()
        for f in range(2):
            z_in[2 * one + f, :, y_rows] = z_out[2 * one + f, me_pz]

    def y_chunk(chunk, _):
        for step in range(1, count_pz):
            z_copy(chunk, step).wait_recv()
        for g in range(0, groups, 2):
            lines = jnp.concatenate([z_in[chunk, g], z_in[chunk, g + 1]], axis=1)
            modes = from_left(left_f[...], lines)
            for h in range(2):
                part = modes[:, h * n : (h + 1) * n].reshape(slabs, count_pz, sub, n)
                swapped = swap_blocks([part[:, b] for b in range(count_pz)], width)
                for block in range(count_pz):
                    start = (block * groups + g + h) * sub
                    y_out[chunk, :, start : start + sub, :] = swapped[block]
        return 0

    def y_forward(one):
        lax.fori_loop(2 * one, 2 * one + 2, y_chunk, 0)

        @pl.when(outer)
        def _():
            for slab in range(slabs):
                for f in range(2):
                    y_copy(2 * one + f, slab).start()

    def square(index):
        freq = jnp.minimum(index, n - index).astype(jnp.float32)
        root = freq * (2.0 * math.pi / n)
        return root * root

    lane = lax.broadcasted_iota(jnp.int32, (1, n), 1)
    ksq_x = square(lax.broadcasted_iota(jnp.int32, (n, 1), 0))
    ksq_z = square(me_pz * width + lane % width)

    def x_both(one, slab):
        for f in range(2):
            y_copy(2 * one + f, slab).wait_recv()
        own_i = me_sp * species + one
        half_stiff = 0.5 * (mobility[own_i, own_i] * kappa[own_i])
        for r in range(0, sub, 2):
            both, ksq = [], []
            for f in range(2):
                chunk = 2 * one + f
                both.append(from_left(half_f[half], jnp.concatenate([
                    jnp.concatenate([
                        field[chunk, slab, pl.ds(r + h, rows_x, stride=sub), :]
                        for field in (y_out, y_in)
                    ], axis=0)
                    for h in range(2)
                ], axis=1)))
            for h in range(2):
                ksq_y = square(slab * slab_ky + (lane // width) * sub + (r + h))
                ksq.append(ksq_x + (ksq_y + ksq_z))
            ksq = jnp.concatenate(ksq, axis=1)
            drop = 0.5 * ksq * (both[0] + ksq * both[1]) / (1.0 + half_stiff * (ksq * ksq))
            lines = from_left(half_i[half], drop)
            for h in range(2):
                rows = pl.ds(r + h, n // 2, stride=sub)
                near[one, slab, rows, :] = lines[: n // 2, h * n : (h + 1) * n]
                x_out[one, slab, rows, :] = lines[n // 2 :, h * n : (h + 1) * n]
        x_copy(one, slab).start()

    def combine(one, slab):
        x_copy(one, slab).wait_recv()
        b_out[one, slab] = near[one, slab, strip:, :] + x_in[one, slab, strip:, :]
        b_copy(one, slab).start()
        b_in[one, slab] = near[one, slab, :strip, :] + x_in[one, slab, :strip, :]

    def y_back(one):
        @pl.when(outer)
        def _():
            for slab in range(slabs):
                b_copy(one, slab).wait_recv()

        for g in range(0, groups, 2):
            pairs = []
            for h in range(2):
                parts = []
                for block in range(count_pz):
                    start = (block * groups + g + h) * sub
                    parts.append(b_in[one, :, start : start + sub, :])
                swapped = swap_blocks(parts, width)
                pairs.append(jnp.stack(swapped, axis=1).reshape(n, n))
            lines = from_left(left_i[...], jnp.concatenate(pairs, axis=1))
            for h in range(2):
                part = lines[:, h * n : (h + 1) * n].reshape(count_pz, rows_y, n)
                w_out[one, :, g + h] = part
        for step in range(1, count_pz):
            w_copy(one, step).start()
        w_in[one, me_pz] = w_out[one, me_pz]

    def z_back(one):
        for step in range(1, count_pz):
            w_copy(one, step).wait_recv()
        for g in range(0, groups, 2):
            rows = []
            for h in range(2):
                rows += swap_blocks([w_in[one, q, g + h] for q in range(count_pz)], width)
            lines = from_right(jnp.concatenate(rows, axis=0), right_i[...])
            lines = lines.reshape(2, count_pz, rows_y, n)
            for h in range(2):
                for block in range(count_pz):
                    x = block * groups + g + h
                    out[one, x] = conc[one, x] - lines[h, block]

    def opening(one, _):
        z_forward(one)

        @pl.when(jnp.logical_and(one >= 1, one <= 2))
        def _():
            y_forward(one - 1)

        return 0

    lax.fori_loop(0, species, opening, 0)
    steps = species * slabs
    lag = 2

    def middle(k, _):
        @pl.when(jnp.logical_and(inner, k < steps))
        def _():
            x_both(k // slabs, lax.rem(k, slabs))

        later = k // slabs + 2

        @pl.when(jnp.logical_and(lax.rem(k, slabs) == 1, later < species))
        def _():
            y_forward(later)

        back = k - lag

        @pl.when(jnp.logical_and(inner, jnp.logical_and(back >= 0, back < steps)))
        def _():
            combine(back // slabs, lax.rem(back, slabs))

        last = jnp.logical_and(back >= 0, lax.rem(k + slabs - lag, slabs) == slabs - 1)

        @pl.when(jnp.logical_and(last, back < steps))
        def _():
            y_back(back // slabs)

        @pl.when(jnp.logical_and(last, back >= slabs))
        def _():
            z_back(back // slabs - 1)

        return 0

    lax.fori_loop(0, steps + slabs + lag, middle, 0)

    for copy in pair:
        copy.wait_send()

    def drain(one, _):
        for step in range(1, count_pz):
            z_copy(2 * one, step).wait_send()
            z_copy(2 * one + 1, step).wait_send()
            w_copy(one, step).wait_send()

        @pl.when(outer)
        def _():
            for slab in range(slabs):
                y_copy(2 * one, slab).wait_send()
                y_copy(2 * one + 1, slab).wait_send()

        @pl.when(inner)
        def _():
            for slab in range(slabs):
                x_copy(one, slab).wait_send()
                b_copy(one, slab).wait_send()

        return 0

    lax.fori_loop(0, species, drain, 0)


def per_device_kernel(concentration, mobility, kappa, well_depth):
    species, rows_x, rows_y, n = concentration.shape
    count_py, count_pz = lax.axis_size("py"), lax.axis_size("pz")
    table = basis(n)
    forward = split_table(table)
    inverse = split_table(table.T)
    blocks = np.arange(n).reshape(count_py, rows_x)
    orders = [blocks[[1, 0, 2, 3]].reshape(n), blocks[[2, 3, 1, 0]].reshape(n)]
    half_forward = np.stack([split_table(table[order[: n // 2]]).T for order in orders])
    half_inverse = np.stack([split_table(table[order].T).T for order in orders])
    depths = jnp.broadcast_to(well_depth[:, None], (species, n))
    groups = rows_x // count_pz
    sub = n // count_py // count_pz
    strip = rows_x * sub
    f32 = jnp.float32
    vmem = pl.BlockSpec(memory_space=pltpu.VMEM)
    smem = pl.BlockSpec(memory_space=pltpu.SMEM)
    dma = pltpu.SemaphoreType.DMA
    return pl.pallas_call(
        functools.partial(kernel, (count_py, count_pz)),
        out_shape=jax.ShapeDtypeStruct(concentration.shape, f32),
        in_specs=[vmem, smem, smem] + [vmem] * 7,
        out_specs=vmem,
        scratch_shapes=[
            pltpu.VMEM((species, rows_x, rows_y, n), f32),
            pltpu.VMEM((species, n), f32),
            pltpu.VMEM((2 * species, count_pz, groups, rows_y, n), f32),
            pltpu.VMEM((2 * species, groups, n, n), f32),
            pltpu.VMEM((2 * species, count_py, strip, n), f32),
            pltpu.VMEM((2 * species, count_py, strip, n), f32),
            pltpu.VMEM((species, count_py, 2 * strip, n), f32),
            pltpu.VMEM((species, count_py, 2 * strip, n), f32),
            pltpu.VMEM((species, count_py, 2 * strip, n), f32),
            pltpu.VMEM((species, count_py, strip, n), f32),
            pltpu.VMEM((species, count_py, strip, n), f32),
            pltpu.VMEM((species, count_pz, groups, rows_y, n), f32),
            pltpu.VMEM((species, count_pz, groups, rows_y, n), f32),
            dma((2,)), dma((2,)),
            dma((2 * species, count_pz)), dma((2 * species, count_pz)),
            dma((2 * species, count_py)), dma((2 * species, count_py)),
            dma((species, count_py)), dma((species, count_py)),
            dma((species, count_py)), dma((species, count_py)),
            dma((species, count_pz)), dma((species, count_pz)),
        ],
        compiler_params=pltpu.CompilerParams(
            collective_id=0, has_side_effects=True, vmem_limit_bytes=60 * 1024 * 1024
        ),
        name="step",
    )(
        concentration, mobility, kappa, depths,
        jnp.asarray(forward), jnp.asarray(inverse),
        jnp.asarray(forward.T), jnp.asarray(inverse.T),
        jnp.asarray(half_forward), jnp.asarray(half_inverse),
    )


def per_device(concentration, mobility, kappa, well_depth):
    rows_x, rows_y, n = concentration.shape[1:]
    count_sp, count_py, count_pz = (lax.axis_size(name) for name in ("sp", "py", "pz"))
    cube = rows_x * count_py == n and rows_y * count_pz == n and n == 128
    power = count_pz > 1 and count_pz & (count_pz - 1) == 0
    whole = n % (8 * count_py * count_pz) == 0 and rows_x % (2 * count_pz) == 0 and rows_y % 8 == 0
    if cube and power and whole and count_sp == 2 and count_py == 4 and concentration.shape[0] > 3:
        return per_device_kernel(concentration, mobility, kappa, well_depth)
    return per_device_general(concentration, mobility, kappa, well_depth)


def solution(mesh):
    in_specs = (P("sp", "py", "pz", None), P(), P(), P("sp"))
    out_specs = P("sp", "py", "pz", None)
    return jax.shard_map(
        per_device, mesh=mesh, in_specs=in_specs, out_specs=out_specs, check_vma=False
    )
```

```python
import functools
import math

import jax
import jax.numpy as jnp
import numpy as np
from jax import lax
from jax.experimental import pallas as pl
from jax.experimental.pallas import tpu as pltpu
from jax.sharding import PartitionSpec as P


def tables(count):
    modes = jnp.arange(count, dtype=jnp.int32)
    product = modes[:, None] * modes[None, :] % count
    angle = 2.0 * math.pi * product.astype(jnp.float32) / count
    return (jnp.cos(angle), jnp.sin(angle))


def wave_square(index, count):
    freq = jnp.where(index < count // 2, index, index - count).astype(jnp.float32)
    return (2.0 * math.pi * freq / count) ** 2


def contract(form, values, table):
    return jnp.einsum(form, values, table, precision=lax.Precision.HIGHEST)


def rotate(spectrum, form, count, forward):
    cosine, sine = tables(count)
    real_part, imag_part = (spectrum[0], spectrum[1])
    real_cos = contract(form, real_part, cosine)
    real_sin = contract(form, real_part, sine)
    imag_cos = contract(form, imag_part, cosine)
    imag_sin = contract(form, imag_part, sine)
    if forward:
        return jnp.stack([real_cos + imag_sin, imag_cos - real_sin])
    return jnp.stack([real_cos - imag_sin, imag_cos + real_sin])


def per_device_general(concentration, mobility, kappa, well_depth):
    local_species, rows_x, rows_y, depth = concentration.shape
    count_sp = lax.axis_size("sp")
    count_py = lax.axis_size("py")
    count_pz = lax.axis_size("pz")
    full_x = rows_x * count_py
    full_y = rows_y * count_pz
    half_depth = depth // 2
    bulk = well_depth[:, None, None, None] * (
        concentration * concentration * concentration - concentration
    )
    fields = jnp.stack([concentration, bulk])
    cosine, sine = tables(depth)
    alternate = (1 - 2 * (jnp.arange(depth, dtype=jnp.int32) % 2)).astype(jnp.float32)
    spectrum = jnp.stack(
        [
            contract("fsxyz,zk->fsxyk", fields, cosine[:, :half_depth]),
            -contract("fsxyz,zk->fsxyk", fields, sine[:, :half_depth]),
        ]
    )
    spectrum = lax.all_to_all(spectrum, "pz", split_axis=5, concat_axis=4, tiled=True)
    own_lines = spectrum.shape[5]
    highest = contract("fsxyz,z->fsxy", fields, alternate)
    highest = lax.all_gather(highest, "pz", axis=3, tiled=True)
    highest = jnp.stack([highest, jnp.zeros_like(highest)])[..., None]
    spectrum = jnp.concatenate([spectrum, highest], axis=5)
    z_modes = jnp.concatenate(
        [
            lax.axis_index("pz") * own_lines + jnp.arange(own_lines, dtype=jnp.int32),
            jnp.full((1,), half_depth, jnp.int32),
        ]
    )
    spectrum = rotate(spectrum, "fsxyz,yk->fsxkz", full_y, True)
    spectrum = lax.all_to_all(
        lax.all_to_all(spectrum, "sp", split_axis=4, concat_axis=2, tiled=True),
        "py",
        split_axis=4,
        concat_axis=3,
        tiled=True,
    )
    spectrum = rotate(spectrum, "fsxyz,xk->fskyz", full_x, True)
    narrow = spectrum.shape[4]
    lines = spectrum.shape[5]
    y_start = (lax.axis_index("sp") * count_py + lax.axis_index("py")) * narrow
    ksq_x = wave_square(jnp.arange(full_x, dtype=jnp.int32), full_x)
    ksq_y = wave_square(y_start + jnp.arange(narrow, dtype=jnp.int32), full_y)
    ksq_z = wave_square(z_modes, depth)
    ksq = ksq_x[:, None, None] + ksq_y[None, :, None] + ksq_z[None, None, :]
    c_hat = spectrum[:, 0]
    drive = spectrum[:, 1] + kappa[None, :, None, None, None] * ksq[None, None] * c_hat
    mix = jnp.einsum("ij,rjxyz->rixyz", mobility, drive, precision=lax.Precision.HIGHEST)
    stiff = 0.5 * (jnp.diagonal(mobility) * kappa)[:, None, None, None] * (ksq * ksq)[None]
    new_hat = (c_hat * (1.0 + stiff)[None] - 0.5 * ksq[None, None] * mix) / (1.0 + stiff)[None]
    new_hat = rotate(new_hat, "sxyz,xk->skyz", full_x, False)
    moved = lax.all_to_all(
        lax.all_to_all(new_hat, "sp", split_axis=1, concat_axis=3, tiled=True),
        "py",
        split_axis=2,
        concat_axis=3,
        tiled=True,
    )
    moved = moved.reshape(2, local_species, rows_x, count_py, count_sp, narrow, lines)
    moved = moved.transpose(0, 1, 2, 4, 3, 5, 6).reshape(2, local_species, rows_x, full_y, lines)
    moved = rotate(moved, "sxyz,yk->sxkz", full_y, False)
    main = moved[..., : lines - 1]
    highest = moved[0, :, :, :, lines - 1]
    main = lax.all_to_all(main, "pz", split_axis=3, concat_axis=4, tiled=True)
    highest = lax.dynamic_slice_in_dim(highest, lax.axis_index("pz") * rows_y, rows_y, 2)
    weight = jnp.where(jnp.arange(half_depth, dtype=jnp.int32) == 0, 1.0, 2.0).astype(jnp.float32)
    result = contract("sxyk,kz->sxyz", main[0] * weight, cosine[:half_depth]) - contract(
        "sxyk,kz->sxyz", main[1] * weight, sine[:half_depth]
    )
    result = result + highest[..., None] * alternate[None, None, None, :]
    return result * (1.0 / (full_x * full_y * depth))


PIECES = 4
SUBLANES = 8


def basis(count):
    grid = np.arange(count)
    mode = np.arange(count)
    freq = np.minimum(mode, count - mode)
    angle = 2.0 * np.pi * (grid[:, None] * freq[None, :] % count) / count
    table = np.where(mode[None, :] <= count // 2, np.cos(angle), np.sin(angle))
    single = (mode == 0) | (2 * mode == count)
    return table * np.sqrt(np.where(single, 1.0, 2.0) / count)[None, :]


def split_table(table):
    table = table.astype(np.float32)
    high = table.astype(jnp.bfloat16)
    low = (table - high.astype(np.float32)).astype(jnp.bfloat16)
    row = np.concatenate([high, low], axis=1)
    return np.concatenate([row, row], axis=0)


def split(values, axis):
    high = values.astype(jnp.bfloat16)
    low = (values - high.astype(jnp.float32)).astype(jnp.bfloat16)
    return jnp.concatenate([high, low], axis=axis)


def from_right(values, table):
    count = values.shape[1]
    out = jnp.dot(split(values, 1), table, preferred_element_type=jnp.float32)
    return out[:, :count] + out[:, count:]


def from_left(table, values):
    count = table.shape[0] // 2
    out = jnp.dot(table, split(values, 0), preferred_element_type=jnp.float32)
    return out[:count] + out[count:]


def swap_blocks(parts, width):
    parts = list(parts)
    axis = parts[0].ndim - 1
    lanes = parts[0].shape[axis]
    block = lax.broadcasted_iota(jnp.int32, parts[0].shape, axis) // width
    half = len(parts) // 2
    while half:
        low_side = (block // half) % 2 == 0
        for first in range(len(parts)):
            if (first // half) % 2 == 0:
                one, two = parts[first], parts[first + half]
                parts[first] = jnp.where(low_side, one, pltpu.roll(two, half * width, axis))
                parts[first + half] = jnp.where(
                    low_side, pltpu.roll(one, lanes - half * width, axis), two
                )
        half //= 2
    return parts


def kernel(
    sizes, conc, mobility, kappa, well_depth, right_f, right_i, left_f, left_i, half_f, half_i, out,
    other, depths, other_depths, z_out, z_in, y_out, y_in, near, x_out, x_in, b_out, b_in, w_out, w_in,
    pair_send, pair_recv, zs, zr, ys, yr, xs, xr, bs, br, ws, wr,
):
    count_py, count_pz = sizes
    species, rows_x, rows_y, n = conc.shape
    me_sp, me_py, me_pz = lax.axis_index("sp"), lax.axis_index("py"), lax.axis_index("pz")
    blocks = count_pz * PIECES
    units = species * PIECES
    width = n // blocks
    groups = rows_x // blocks
    sub = SUBLANES
    slab_ky = blocks * sub
    slabs = n // slab_ky
    strip = rows_x * sub
    mesh_id = pl.DeviceIdType.MESH

    half = me_py // 2
    inner = lax.rem(me_py + half, 2) == 1
    outer = jnp.logical_not(inner)
    buddy = {"sp": me_sp, "py": me_py + 1 - 2 * lax.rem(me_py, 2), "pz": me_pz}
    across = {"sp": me_sp, "py": count_py - 1 - me_py, "pz": me_pz}

    def along_pz(step):
        return {"sp": me_sp, "py": me_py, "pz": lax.rem(me_pz + step, count_pz)}

    partner = {"sp": 1 - me_sp, "py": me_py, "pz": me_pz}
    barrier = pltpu.get_barrier_semaphore()
    peers = [partner, buddy]
    peers += [along_pz(step) for step in range(1, count_pz)]
    for peer in peers:
        pl.semaphore_signal(barrier, inc=1, device_id=peer, device_id_type=mesh_id)

    @pl.when(inner)
    def _():
        pl.semaphore_signal(barrier, inc=1, device_id=across, device_id_type=mesh_id)

    for t in range(species):
        depths[t : t + 1, :] = jnp.full((1, n), well_depth[t], jnp.float32)
    pl.semaphore_wait(barrier, len(peers) + jnp.where(inner, 1, 0))

    def remote(source, target, send, recv, peer):
        return pltpu.make_async_remote_copy(
            src_ref=source, dst_ref=target, send_sem=send, recv_sem=recv,
            device_id=peer, device_id_type=mesh_id,
        )

    pair = [
        remote(depths, other_depths, pair_send.at[0], pair_recv.at[0], partner),
        remote(conc, other, pair_send.at[1], pair_recv.at[1], partner),
    ]
    for copy in pair:
        copy.start()

    y_rows = pl.ds(pl.multiple_of(me_pz * rows_y, rows_y), rows_y)

    def z_copy(chunk, step):
        peer = lax.rem(me_pz + step, count_pz)
        return remote(
            z_out.at[chunk, peer], z_in.at[chunk, :, y_rows], zs.at[chunk, step],
            zr.at[chunk, step], along_pz(step),
        )

    def y_copy(chunk, slab):
        return remote(
            y_out.at[chunk, slab], y_in.at[chunk, slab], ys.at[chunk, slab],
            yr.at[chunk, slab], buddy,
        )

    def x_copy(one, slab):
        return remote(
            x_out.at[one, slab], x_in.at[one, slab], xs.at[one, slab], xr.at[one, slab], across
        )

    def b_copy(one, slab):
        return remote(
            b_out.at[one, slab], b_in.at[one, slab], bs.at[one, slab], br.at[one, slab], buddy
        )

    def w_copy(one, step):
        peer = lax.rem(me_pz + step, count_pz)
        return remote(
            w_out.at[one, peer], w_in.at[one, me_pz], ws.at[one, step],
            wr.at[one, step], along_pz(step),
        )

    for copy in pair:
        copy.wait_recv()

    def z_forward(one):
        own_i = me_sp * species + one
        terms = []
        for side, field, depth in ((me_sp, conc, depths), (1 - me_sp, other, other_depths)):
            for t in range(species):
                j = side * species + t
                weight = mobility[own_i, j]
                terms.append((field, t, weight * depth[t : t + 1, :], weight * kappa[j]))
        for g in range(groups):
            bulk_mix, conc_mix = [], []
            for block in range(blocks):
                first = second = None
                for field, t, bulk_weight, conc_weight in terms:
                    c = field[t, block * groups + g]
                    a = bulk_weight * (c * c * c - c)
                    b = conc_weight * c
                    first = a if first is None else first + a
                    second = b if second is None else second + b
                bulk_mix.append(first)
                conc_mix.append(second)
            modes = from_right(jnp.concatenate(bulk_mix + conc_mix, axis=0), right_f[...])
            modes = modes.reshape(2, blocks, rows_y, n)
            for f in range(2):
                swapped = swap_blocks([modes[f, block] for block in range(blocks)], width)
                for block in range(blocks):
                    unit = PIECES * one + block % PIECES
                    z_out[2 * unit + f, block // PIECES, g] = swapped[block]
        for c in range(2 * PIECES):
            for step in range(1, count_pz):
                z_copy(2 * PIECES * one + c, step).start()
        for c in range(2 * PIECES):
            chunk = 2 * PIECES * one + c
            z_in[chunk, :, y_rows] = z_out[chunk, me_pz]

    def y_chunk(chunk, _):
        for step in range(1, count_pz):
            z_copy(chunk, step).wait_recv()
        for g in range(0, groups, 2):
            lines = jnp.concatenate([z_in[chunk, g], z_in[chunk, g + 1]], axis=1)
            modes = from_left(left_f[...], lines)
            for h in range(2):
                part = modes[:, h * n : (h + 1) * n].reshape(slabs, blocks, sub, n)
                swapped = swap_blocks([part[:, b] for b in range(blocks)], width)
                for block in range(blocks):
                    start = (block * groups + g + h) * sub
                    y_out[chunk, :, start : start + sub, :] = swapped[block]
        return 0

    def y_forward(one):
        lax.fori_loop(2 * one, 2 * one + 2, y_chunk, 0)

        @pl.when(outer)
        def _():
            for slab in range(slabs):
                for f in range(2):
                    y_copy(2 * one + f, slab).start()

    def square(index):
        freq = jnp.minimum(index, n - index).astype(jnp.float32)
        root = freq * (2.0 * math.pi / n)
        return root * root

    lane = lax.broadcasted_iota(jnp.int32, (1, n), 1)
    ksq_x = square(lax.broadcasted_iota(jnp.int32, (n, 1), 0))

    def x_both(one, slab):
        for f in range(2):
            y_copy(2 * one + f, slab).wait_recv()
        own_i = me_sp * species + one // PIECES
        piece = me_pz * PIECES + lax.rem(one, PIECES)
        ksq_z = square(piece * width + lane % width)
        half_stiff = 0.5 * (mobility[own_i, own_i] * kappa[own_i])
        for r in range(0, sub, 2):
            both, ksq = [], []
            for f in range(2):
                chunk = 2 * one + f
                both.append(from_left(half_f[half], jnp.concatenate([
                    jnp.concatenate([
                        field[chunk, slab, pl.ds(r + h, rows_x, stride=sub), :]
                        for field in (y_out, y_in)
                    ], axis=0)
                    for h in range(2)
                ], axis=1)))
            for h in range(2):
                ksq_y = square(slab * slab_ky + (lane // width) * sub + (r + h))
                ksq.append(ksq_x + (ksq_y + ksq_z))
            ksq = jnp.concatenate(ksq, axis=1)
            drop = 0.5 * ksq * (both[0] + ksq * both[1]) / (1.0 + half_stiff * (ksq * ksq))
            lines = from_left(half_i[half], drop)
            for h in range(2):
                rows = pl.ds(r + h, n // 2, stride=sub)
                near[one, slab, rows, :] = lines[: n // 2, h * n : (h + 1) * n]
                x_out[one, slab, rows, :] = lines[n // 2 :, h * n : (h + 1) * n]
        x_copy(one, slab).start()

    def combine(one, slab):
        x_copy(one, slab).wait_recv()
        b_out[one, slab] = near[one, slab, strip:, :] + x_in[one, slab, strip:, :]
        b_copy(one, slab).start()
        b_in[one, slab] = near[one, slab, :strip, :] + x_in[one, slab, :strip, :]

    def y_back(one):
        @pl.when(outer)
        def _():
            for slab in range(slabs):
                b_copy(one, slab).wait_recv()

        for g in range(0, groups, 2):
            pairs = []
            for h in range(2):
                parts = []
                for block in range(blocks):
                    start = (block * groups + g + h) * sub
                    parts.append(b_in[one, :, start : start + sub, :])
                swapped = swap_blocks(parts, width)
                pairs.append(jnp.stack(swapped, axis=1).reshape(n, n))
            lines = from_left(left_i[...], jnp.concatenate(pairs, axis=1))
            for h in range(2):
                part = lines[:, h * n : (h + 1) * n].reshape(count_pz, rows_y, n)
                w_out[one, :, g + h] = part
        for step in range(1, count_pz):
            w_copy(one, step).start()
        w_in[one, me_pz] = w_out[one, me_pz]

    def z_back(one):
        for c in range(PIECES):
            for step in range(1, count_pz):
                w_copy(PIECES * one + c, step).wait_recv()
        for g in range(0, groups, 2):
            rows = []
            for h in range(2):
                rows += swap_blocks([
                    w_in[PIECES * one + block % PIECES, block // PIECES, g + h]
                    for block in range(blocks)
                ], width)
            lines = from_right(jnp.concatenate(rows, axis=0), right_i[...])
            lines = lines.reshape(2, blocks, rows_y, n)
            for h in range(2):
                for block in range(blocks):
                    x = block * groups + g + h
                    out[one, x] = conc[one, x] - lines[h, block]

    z_forward(0)
    y_forward(0)

    def opening(one, _):
        z_forward(one)
        return 0

    lax.fori_loop(1, species, opening, 0)
    y_forward(1)
    steps = units * slabs
    lag = 2

    def middle(k, _):
        @pl.when(jnp.logical_and(inner, k < steps))
        def _():
            x_both(k // slabs, lax.rem(k, slabs))

        for ahead in range(2):
            later = 2 * k + 2 + ahead

            @pl.when(later < units)
            def _():
                y_forward(later)

        back = k - lag

        @pl.when(jnp.logical_and(inner, jnp.logical_and(back >= 0, back < steps)))
        def _():
            combine(back // slabs, lax.rem(back, slabs))

        full = jnp.logical_and(back >= 0, lax.rem(back + 1, slabs) == 0)

        @pl.when(jnp.logical_and(full, back < steps))
        def _():
            y_back(back // slabs)

        done = back - 2 * slabs + 1
        whole = jnp.logical_and(done > 0, lax.rem(done, PIECES * slabs) == 0)

        @pl.when(whole)
        def _():
            z_back(done // (PIECES * slabs) - 1)

        return 0

    lax.fori_loop(0, steps + lag + 2 * slabs, middle, 0)

    for copy in pair:
        copy.wait_send()

    def drain(one, _):
        for step in range(1, count_pz):
            z_copy(2 * one, step).wait_send()
            z_copy(2 * one + 1, step).wait_send()
            w_copy(one, step).wait_send()

        @pl.when(outer)
        def _():
            for slab in range(slabs):
                y_copy(2 * one, slab).wait_send()
                y_copy(2 * one + 1, slab).wait_send()

        @pl.when(inner)
        def _():
            for slab in range(slabs):
                x_copy(one, slab).wait_send()
                b_copy(one, slab).wait_send()

        return 0

    lax.fori_loop(0, units, drain, 0)


def per_device_kernel(concentration, mobility, kappa, well_depth):
    species, rows_x, rows_y, n = concentration.shape
    count_py, count_pz = lax.axis_size("py"), lax.axis_size("pz")
    table = basis(n)
    forward = split_table(table)
    inverse = split_table(table.T)
    blocks = np.arange(n).reshape(count_py, rows_x)
    orders = [blocks[[1, 0, 2, 3]].reshape(n), blocks[[2, 3, 1, 0]].reshape(n)]
    half_forward = np.stack([split_table(table[order[: n // 2]]).T for order in orders])
    half_inverse = np.stack([split_table(table[order].T).T for order in orders])
    blocks = count_pz * PIECES
    units = species * PIECES
    groups = rows_x // blocks
    slabs = n // (blocks * SUBLANES)
    strip = rows_x * SUBLANES
    f32 = jnp.float32
    vmem = pl.BlockSpec(memory_space=pltpu.VMEM)
    smem = pl.BlockSpec(memory_space=pltpu.SMEM)
    dma = pltpu.SemaphoreType.DMA
    return pl.pallas_call(
        functools.partial(kernel, (count_py, count_pz)),
        out_shape=jax.ShapeDtypeStruct(concentration.shape, f32),
        in_specs=[vmem, smem, smem, smem] + [vmem] * 6,
        out_specs=vmem,
        scratch_shapes=[
            pltpu.VMEM((species, rows_x, rows_y, n), f32),
            pltpu.VMEM((species, n), f32),
            pltpu.VMEM((species, n), f32),
            pltpu.VMEM((2 * units, count_pz, groups, rows_y, n), f32),
            pltpu.VMEM((2 * units, groups, n, n), f32),
            pltpu.VMEM((2 * units, slabs, strip, n), f32),
            pltpu.VMEM((2 * units, slabs, strip, n), f32),
            pltpu.VMEM((units, slabs, 2 * strip, n), f32),
            pltpu.VMEM((units, slabs, 2 * strip, n), f32),
            pltpu.VMEM((units, slabs, 2 * strip, n), f32),
            pltpu.VMEM((units, slabs, strip, n), f32),
            pltpu.VMEM((units, slabs, strip, n), f32),
            pltpu.VMEM((units, count_pz, groups, rows_y, n), f32),
            pltpu.VMEM((units, count_pz, groups, rows_y, n), f32),
            dma((2,)), dma((2,)),
            dma((2 * units, count_pz)), dma((2 * units, count_pz)),
            dma((2 * units, slabs)), dma((2 * units, slabs)),
            dma((units, slabs)), dma((units, slabs)),
            dma((units, slabs)), dma((units, slabs)),
            dma((units, count_pz)), dma((units, count_pz)),
        ],
        compiler_params=pltpu.CompilerParams(
            collective_id=0, has_side_effects=True, vmem_limit_bytes=60 * 1024 * 1024
        ),
        name="step",
    )(
        concentration, mobility, kappa, well_depth,
        jnp.asarray(forward), jnp.asarray(inverse),
        jnp.asarray(forward.T), jnp.asarray(inverse.T),
        jnp.asarray(half_forward), jnp.asarray(half_inverse),
    )


def per_device(concentration, mobility, kappa, well_depth):
    rows_x, rows_y, n = concentration.shape[1:]
    count_sp, count_py, count_pz = (lax.axis_size(name) for name in ("sp", "py", "pz"))
    cube = rows_x * count_py == n and rows_y * count_pz == n and n == 128
    power = count_pz > 1 and count_pz & (count_pz - 1) == 0
    blocks = count_pz * PIECES
    whole = n % (SUBLANES * blocks) == 0 and rows_x % (2 * blocks) == 0 and rows_y % SUBLANES == 0
    if cube and power and whole and count_sp == 2 and count_py == 4:
        return per_device_kernel(concentration, mobility, kappa, well_depth)
    return per_device_general(concentration, mobility, kappa, well_depth)


def solution(mesh):
    in_specs = (P("sp", "py", "pz", None), P(), P(), P("sp"))
    out_specs = P("sp", "py", "pz", None)
    return jax.shard_map(
        per_device, mesh=mesh, in_specs=in_specs, out_specs=out_specs, check_vma=False
    )
```
